32 devices in a mesh: group: 16 (over z, y, core), helper: 2 (over x).
Axes of the slice: x: 2, y: 2, z: 4, core: 2. Of those that a mesh axis runs over, the one named last changes fastest.
Arguments:
- candidates: bfloat16 [16, 512, 1024], P('group', 'helper'), may hold values from -6 to 6
- prefix_cache: bfloat16 [16, 2, 768, 1024], P('group', None, 'helper'), may hold values from -6 to 6
- w_uvqk: bfloat16 [1024, 4096], replicated, may hold values from -0.1875 to 0.1875
- w_output: bfloat16 [1024, 1024], replicated, may hold values from -0.1875 to 0.1875
- norm_gain: float32 [1024], replicated, may hold values from 0.1 to 1.9
- owner: int32 [16], replicated, may hold values from 0 to 15, as said below
- counts: int32 [16], replicated, may hold values from 256 to 512, as said below
- prefix_len: int32 [16], replicated, may hold values from 24 to 768, as said below
Outputs:
- update: bfloat16 [16, 512, 1024], P('group', 'helper')
The draws below stay inside these ranges and needn't reach their ends.
Inputs may be any that keep to these rules, and one draw needn't show every extreme that they name: owner[u] = (u + s) mod 16 for one shift s of the round. `counts`: multiples of 128; some user has exactly 512. `prefix_len`: some user has exactly 768.
All inputs are finite; a program needn't handle non-finite values.
Results may differ from the reference program's by a relative error of at most 0.012.
Values may be sent and summed in bfloat16 or wider, within the bound.
A program may use at most 128 MiB of HBM per device.

```python
import jax
import jax.numpy as jnp
from jax import lax

D = 1024
HEADS = 8
PREFIX = 768
CAND = 512
GRAIN = 128
USERS = 16


def draw_owner(key, part):
    offset = jax.random.randint(key, (), 0, USERS)
    return ((jnp.arange(USERS, dtype=jnp.int32) + offset) % USERS).astype(jnp.int32)


def draw_counts(key, part):
    first, second = jax.random.split(jax.random.fold_in(key, 11))
    steps = jax.random.randint(first, (USERS,), CAND // (2 * GRAIN), CAND // GRAIN + 1)
    chosen = jax.random.randint(second, (), 0, USERS)
    values = jnp.where(jnp.arange(USERS) == chosen, CAND, steps * GRAIN)
    return values.astype(jnp.int32)


def draw_prefix_len(key, part):
    first, second = jax.random.split(jax.random.fold_in(key, 23))
    values = jax.random.randint(first, (USERS,), max(1, PREFIX // 32), PREFIX + 1)
    chosen = jax.random.randint(second, (), 0, USERS)
    values = jnp.where(jnp.arange(USERS) == chosen, PREFIX, values)
    return values.astype(jnp.int32)


def block_levels(own_key, dims, shards, smallest, high):
    def one(position, blocks):
        draws = jax.random.uniform(jax.random.fold_in(jax.random.fold_in(own_key, 6), position), (blocks,), jnp.float32, smallest / len(shards), high / len(shards))
        return jnp.repeat(jnp.exp(draws), dims[position] // blocks).reshape((-1,) + (1,) * (len(dims) - position - 1))

    factor_of = one(*shards[0])
    for cut in shards[1:]:
        factor_of = factor_of * one(*cut)
    return factor_of


def noise(stream_key, shape, scale, most, cuts=(), kind=jnp.bfloat16):
    level = block_levels(stream_key, shape, cuts, -0.22, 0.18) if cuts else 1.0
    values = jax.random.normal(stream_key, shape, jnp.float32) * scale * level
    return jnp.minimum(jnp.maximum(values, -most), most).astype(kind)


def setup_inputs(seed: int = 0) -> dict:
    seeds = jax.random.split(jax.random.key(seed), 9)
    candidates = noise(seeds[0], (USERS, CAND, D), 1.0, 6.0, ((0, 16), (1, 2)))
    prefix_cache = noise(seeds[1], (USERS, 2, PREFIX, D), 1.0, 6.0, ((0, 16), (2, 2)))
    w_uvqk = noise(seeds[2], (D, 4 * D), D ** -0.5, 0.1875)
    w_output = noise(seeds[3], (D, D), D ** -0.5, 0.1875)
    norm_gain = jnp.clip(1.0 + 0.18 * jax.random.normal(seeds[4], (D,), jnp.float32), 0.1, 1.9)
    owner = draw_owner(jax.random.fold_in(seeds[8], 71), 0)
    counts = draw_counts(jax.random.fold_in(seeds[8], 71), 0)
    prefix_len = draw_prefix_len(jax.random.fold_in(seeds[8], 71), 0)
    return dict(candidates=candidates, prefix_cache=prefix_cache, w_uvqk=w_uvqk, w_output=w_output, norm_gain=norm_gain, owner=owner, counts=counts, prefix_len=prefix_len)


def score_user(rows, keys, values, count, visible, w_uvqk, w_output, norm_gain):
    width = rows.shape[1]
    head = width // HEADS
    scale = head ** (-0.5)
    total = rows.shape[0]
    proj = jax.nn.silu(jnp.dot(rows, w_uvqk, preferred_element_type=jnp.float32))
    gate_u = proj[:, :width]
    own_v = proj[:, width:2 * width].astype(jnp.bfloat16).astype(jnp.float32).reshape(total, HEADS, head)
    query = proj[:, 2 * width:3 * width].astype(jnp.bfloat16).astype(jnp.float32).reshape(total, HEADS, head)
    own_k = proj[:, 3 * width:].astype(jnp.bfloat16).astype(jnp.float32).reshape(total, HEADS, head)
    length = keys.shape[0]
    keys4 = keys.astype(jnp.float32).reshape(length, HEADS, head)
    values4 = values.astype(jnp.float32).reshape(length, HEADS, head)
    scores = jnp.einsum('rhd,nhd->hrn', query, keys4) * scale
    allowed = jnp.arange(length, dtype=jnp.int32) < visible
    weights = jnp.where(allowed[None, None, :], jax.nn.silu(scores), 0.0).astype(jnp.bfloat16).astype(jnp.float32)
    mixed = jnp.einsum('hrn,nhd->rhd', weights, values4)
    selfw = jax.nn.silu(lax.optimization_barrier(jnp.sum(query * own_k, axis=-1)) * scale).astype(jnp.bfloat16).astype(jnp.float32)
    mixed = (mixed + selfw[:, :, None] * own_v).reshape(total, width)
    centre = mixed - lax.optimization_barrier(jnp.mean(mixed, axis=-1, keepdims=True))
    spread = lax.optimization_barrier(jnp.mean(centre * centre, axis=-1, keepdims=True))
    normed = (centre * lax.rsqrt(spread + 1e-05) * norm_gain * gate_u).astype(jnp.bfloat16)
    result = jnp.dot(normed, w_output, preferred_element_type=jnp.float32)
    live = jnp.arange(total, dtype=jnp.int32) < count
    return jnp.where(live[:, None], result, 0.0).astype(jnp.bfloat16)

def reference(candidates, prefix_cache, w_uvqk, w_output, norm_gain, owner, counts, prefix_len):
    shift = owner[0]

    def one_user(user):
        rows = lax.dynamic_index_in_dim(candidates, user, 0, keepdims=False)
        source = ((user + shift) % USERS).astype(jnp.int32)
        cache = lax.dynamic_index_in_dim(prefix_cache, source, 0, keepdims=False)
        count = lax.dynamic_index_in_dim(counts, user, 0, keepdims=False)
        visible = lax.dynamic_index_in_dim(prefix_len, user, 0, keepdims=False)
        return score_user(rows, cache[0], cache[1], count, visible, w_uvqk, w_output, norm_gain)
    result = lax.map(one_user, jnp.arange(USERS, dtype=jnp.int32))
    return jnp.roll(result, shift, axis=0)
```

```python
import functools
import math

import jax
import jax.numpy as jnp
from jax import lax
from jax.experimental import pallas as pl
from jax.experimental.pallas import tpu as pltpu
from jax.sharding import PartitionSpec as P

HEADS = 8
EPS = 1e-05
CHUNKS = 4
MESH = pl.DeviceIdType.MESH


def silu(v):
    t = v * 0.5
    return t + t * jnp.tanh(t)


def attend(query, keys, values, scale):
    scores = lax.dot_general(
        query, keys, (((1,), (1,)), ((), ())), preferred_element_type=jnp.float32
    )
    t = scores * (0.5 * scale)
    weights = (t + t * jnp.tanh(t)).astype(jnp.bfloat16)
    return jnp.dot(weights, values, preferred_element_type=jnp.float32)


def seen(values, base, visible):
    rows = lax.broadcasted_iota(jnp.int32, values.shape, 0) + base
    return jnp.where(rows < visible, values, jnp.zeros_like(values))


def plan(shift, groups):
    return dict(kv_heads=2, lag=1, end_lag=2)


def layer_kernel(
    shift, chunks, kv_heads, lag, end_lag,
    owner, counts, prefix_len, cand, cache, w, w_out, gain, out,
    tok, wq, kv, vm, pk, q, pq, ans, got, u, acc, wo, gn, staged,
    w_sems, kv_sem, wo_sem, gn_sem, out_sems,
    tok_send, tok_recv, pk_send, pk_recv, q_send, q_recv, a_send, a_recv,
):
    groups = lax.axis_size("group")
    helpers = lax.axis_size("helper")
    g = lax.axis_index("group")
    h = lax.axis_index("helper")
    slots, width = cand.shape
    length = cache.shape[1]
    head = width // HEADS
    scale = head ** (-0.5)
    size = slots // chunks
    wide = 2 * head
    pairs = width // wide
    sent_pairs = kv_heads // 2
    q_pairs = pairs - sent_pairs
    q_width = q_pairs * wide
    others = list(range(1, helpers))
    user = lax.rem(g - shift + groups, groups)
    visible = prefix_len[user]
    live = counts[user] - h * slots

    loads = []
    for n, k in enumerate((2, 3, 1, 0)):
        cols = slice(k * width, (k + 1) * width)
        loads.append(pltpu.make_async_copy(w.at[:, cols], wq.at[k], w_sems.at[n]))
    loads[0].start()
    kv_load = pltpu.make_async_copy(cache, kv, kv_sem)
    kv_load.start()
    for load in loads[1:]:
        load.start()
    wo_load = pltpu.make_async_copy(w_out, wo, wo_sem)
    wo_load.start()
    gn_load = pltpu.make_async_copy(gain, gn, gn_sem)
    gn_load.start()

    barrier = pltpu.get_barrier_semaphore()
    friends = [{"helper": lax.rem(h + away, helpers)} for away in others]
    if shift:
        target = lax.rem(g + shift, groups)
        friends.append({"group": target})
        friends.append({"group": user})
    for friend in friends:
        pl.semaphore_signal(barrier, inc=1, device_id=friend, device_id_type=MESH)
    pl.semaphore_wait(barrier, len(friends))

    def part(c):
        return pl.ds(pl.multiple_of(c * size, size), size)

    def token_copy(c):
        rows = part(c)
        if not shift:
            return pltpu.make_async_copy(cand.at[rows], tok.at[rows], tok_recv.at[c])
        return pltpu.make_async_remote_copy(
            cand.at[rows], tok.at[rows], tok_send.at[c], tok_recv.at[c],
            device_id={"group": target}, device_id_type=MESH,
        )

    for c in range(chunks):
        token_copy(c).start()

    def kv_copy(n, away, kind):
        cols = slice(q_width + n * wide, q_width + (n + 1) * wide)
        here = slice(n * wide, (n + 1) * wide)
        return pltpu.make_async_remote_copy(
            cache.at[kind, :, cols], pk.at[away - 1, kind, :, here],
            pk_send.at[away - 1, kind, n], pk_recv.at[away - 1, kind, n],
            device_id={"helper": lax.rem(h + away, helpers)}, device_id_type=MESH,
        )

    kv_copies = [kv_copy(n, away, kind) for n in range(sent_pairs) for away in others for kind in (0, 1)]
    for copy in kv_copies:
        copy.start()

    def query_copy(away, c):
        rows = part(c)
        return pltpu.make_async_remote_copy(
            q.at[rows, 0:q_width], pq.at[away - 1, rows, :],
            q_send.at[away - 1, c], q_recv.at[away - 1, c],
            device_id={"helper": lax.rem(h + away, helpers)}, device_id_type=MESH,
        )

    def answer_copy(away, c):
        rows = part(c)
        return pltpu.make_async_remote_copy(
            ans.at[away - 1, rows, :], got.at[away - 1, rows, :],
            a_send.at[away - 1, c], a_recv.at[away - 1, c],
            device_id={"helper": lax.rem(h - away + helpers, helpers)}, device_id_type=MESH,
        )

    def at_pair(n):
        return pl.ds(pl.multiple_of(n * wide, wide), wide)

    def project(k, rows, cols):
        return silu(jnp.dot(tok[rows, :], wq[k, :, cols], preferred_element_type=jnp.float32))

    def queries(c):
        rows = part(c)

        def body(n, _):
            cols = at_pair(n)
            q[rows, cols] = project(2, rows, cols).astype(jnp.bfloat16)
            return 0

        lax.fori_loop(0, q_pairs, body, 0)
        for away in others:
            query_copy(away, c).start()
        if sent_pairs:
            lax.fori_loop(q_pairs, pairs, body, 0)

    def own(c):
        rows = part(c)

        def body(n, _):
            cols = at_pair(n)
            query = q[rows, cols]
            own_k = project(3, rows, cols).astype(jnp.bfloat16).astype(jnp.float32)
            own_v = project(1, rows, cols).astype(jnp.bfloat16).astype(jnp.float32)
            u[rows, cols] = project(0, rows, cols)
            prod = query.astype(jnp.float32) * own_k
            keys = kv[0, :, cols]
            values = vm[:, cols]
            sums = []
            for m in range(2):
                here = slice(m * head, (m + 1) * head)
                selfw = silu(jnp.sum(prod[:, here], axis=1, keepdims=True) * scale)
                selfw = selfw.astype(jnp.bfloat16).astype(jnp.float32)
                mixed = attend(query[:, here], keys[:, here], values[:, here], scale)
                sums.append(mixed + selfw * own_v[:, here])
            acc[rows, cols] = jnp.concatenate(sums, axis=1)
            return 0

        lax.fori_loop(0, pairs, body, 0)

    def answers(c):
        rows = part(c)
        for away in others:
            query_copy(away, c).wait_recv()

            def body(n, _):
                cols = at_pair(n)
                query = pq[away - 1, rows, cols]
                keys = kv[0, :, cols]
                values = vm[:, cols]
                sums = []
                for m in range(2):
                    here = slice(m * head, (m + 1) * head)
                    sums.append(attend(query[:, here], keys[:, here], values[:, here], scale))
                ans[away - 1, rows, cols] = jnp.concatenate(sums, axis=1).astype(jnp.bfloat16)
                return 0

            lax.fori_loop(0, q_pairs, body, 0)
            answer_copy(away, c).start()

    def traveled(c):
        rows = part(c)
        for n in range(sent_pairs):
            cols = slice(q_width + n * wide, q_width + (n + 1) * wide)
            query = q[rows, cols]
            total = acc[rows, cols]
            sums = [total[:, :head], total[:, head:]]
            for away in others:
                base = lax.rem(h - away + helpers, helpers) * length
                keys = pk[away - 1, 0, :, n * wide:(n + 1) * wide]
                values = seen(pk[away - 1, 1, :, n * wide:(n + 1) * wide], base, visible)
                for m in range(2):
                    here = slice(m * head, (m + 1) * head)
                    sums[m] += attend(query[:, here], keys[:, here], values[:, here], scale)
            acc[rows, cols] = jnp.concatenate(sums, axis=1)

    def finish(c):
        rows = part(c)
        if sent_pairs:
            traveled(c)
        for away in others:
            answer_copy(away, c).wait_recv()
        a = acc[rows, :]
        gate = u[rows, :]
        for away in others:
            extra = got[away - 1, rows, :].astype(jnp.float32)
            if sent_pairs:
                extra = jnp.concatenate([extra, jnp.zeros((size, width - q_width), jnp.float32)], axis=1)
            a += extra
        centre = a - jnp.mean(a, axis=-1, keepdims=True)
        spread = jnp.mean(centre * centre, axis=-1, keepdims=True)
        normed = (centre * lax.rsqrt(spread + EPS) * gn[...] * gate).astype(jnp.bfloat16)

        def body(n, _):
            cols = at_pair(n)
            result = jnp.dot(normed, wo[:, cols], preferred_element_type=jnp.float32)
            places = lax.broadcasted_iota(jnp.int32, result.shape, 0) + c * size
            staged[rows, cols] = jnp.where(places < live, result, 0.0).astype(jnp.bfloat16)
            return 0

        lax.fori_loop(0, pairs, body, 0)
        out_copy(c).start()

    def out_copy(c):
        rows = part(c)
        return pltpu.make_async_copy(staged.at[rows], out.at[rows], out_sems.at[c])

    def mask(n, _):
        cols = at_pair(n)
        vm[:, cols] = seen(kv[1, :, cols], h * length, visible)
        return 0

    def step(t, _):
        @pl.when(t < chunks)
        def _():
            token_copy(t).wait_recv() if shift else token_copy(t).wait()

            @pl.when(t == 0)
            def _():
                loads[0].wait()

            queries(t)

            @pl.when(t == 0)
            def _():
                kv_load.wait()
                lax.fori_loop(0, pairs, mask, 0)
                for load in loads[1:]:
                    load.wait()

            own(t)

        late = t - lag

        @pl.when(jnp.logical_and(late >= 0, late < chunks))
        def _():
            answers(late)

        last = t - end_lag

        @pl.when(last >= 0)
        def _():
            @pl.when(last == 0)
            def _():
                for copy in kv_copies:
                    copy.wait_recv()
                wo_load.wait()
                gn_load.wait()

            finish(last)

        return 0

    lax.fori_loop(0, chunks + end_lag, step, 0)

    def drain(c, _):
        if shift:
            token_copy(c).wait_send()
        for away in others:
            query_copy(away, c).wait_send()
            answer_copy(away, c).wait_send()
        out_copy(c).wait()
        return 0

    lax.fori_loop(0, chunks, drain, 0)
    for copy in kv_copies:
        copy.wait_send()


def layer(shift, groups, helpers, owner, counts, prefix_len, cand, cache, w, w_out, gain):
    slots, width = cand.shape
    length = cache.shape[1]
    chunks = CHUNKS
    setup = plan(shift, groups)
    kv_heads = setup["kv_heads"]
    q_width = width - kv_heads * (width // HEADS)
    pieces = helpers - 1
    kv_width = max(width - q_width, 128)
    dma = pltpu.SemaphoreType.DMA
    smem = pl.BlockSpec(memory_space=pltpu.SMEM)
    anywhere = pl.BlockSpec(memory_space=pl.ANY)
    bf16, f32 = jnp.bfloat16, jnp.float32
    return pl.pallas_call(
        functools.partial(layer_kernel, shift, chunks, kv_heads, setup["lag"], setup["end_lag"]),
        in_specs=[smem] * 3 + [anywhere] * 5,
        out_specs=anywhere,
        out_shape=jax.ShapeDtypeStruct((slots, width), bf16),
        scratch_shapes=[
            pltpu.VMEM((slots, width), bf16),
            pltpu.VMEM((4, width, width), bf16),
            pltpu.VMEM((2, length, width), bf16),
            pltpu.VMEM((length, width), bf16),
            pltpu.VMEM((pieces, 2, length, kv_width), bf16),
            pltpu.VMEM((slots, width), bf16),
            pltpu.VMEM((pieces, slots, q_width), bf16),
            pltpu.VMEM((pieces, slots, q_width), bf16),
            pltpu.VMEM((pieces, slots, q_width), bf16),
            pltpu.VMEM((slots, width), f32),
            pltpu.VMEM((slots, width), f32),
            pltpu.VMEM((width, width), bf16),
            pltpu.VMEM((1, width), f32),
            pltpu.VMEM((slots, width), bf16),
            dma((4,)), dma(()), dma(()), dma(()), dma((chunks,)),
            dma((chunks,)), dma((chunks,)),
            dma((pieces, 2, max(kv_heads // 2, 1))), dma((pieces, 2, max(kv_heads // 2, 1))),
            dma((pieces, chunks)), dma((pieces, chunks)),
            dma((pieces, chunks)), dma((pieces, chunks)),
        ],
        compiler_params=pltpu.CompilerParams(
            collective_id=shift, has_side_effects=True, vmem_limit_bytes=60 * 1024 * 1024
        ),
        name="layer",
    )(owner, counts, prefix_len, cand, cache, w, w_out, gain)


def local(candidates, prefix_cache, w_uvqk, w_output, norm_gain, owner, counts, prefix_len):
    groups = lax.axis_size("group")
    helpers = lax.axis_size("helper")
    _, slots, width = candidates.shape
    length = prefix_cache.shape[2]
    cache = prefix_cache.reshape(2, length, width)
    branches = [functools.partial(layer, s, groups, helpers) for s in range(groups)]
    result = lax.switch(
        owner[0], branches, owner, counts, prefix_len,
        candidates[0], cache, w_uvqk, w_output, norm_gain.reshape(1, width),
    )
    return result[None]


def solution(mesh):
    in_specs = (
        P("group", "helper", None),
        P("group", None, "helper", None),
        P(),
        P(),
        P(),
        P(),
        P(),
        P(),
    )
    out_specs = P("group", "helper", None)
    return jax.shard_map(local, mesh=mesh, in_specs=in_specs, out_specs=out_specs, check_vma=False)
```

```python
import functools

import jax
import jax.numpy as jnp
from jax import lax
from jax.experimental import pallas as pl
from jax.experimental.pallas import tpu as pltpu
from jax.sharding import PartitionSpec as P

HEADS = 8
EPS = 1e-05
MESH = pl.DeviceIdType.MESH


def silu(v):
    t = v * 0.5
    return t + t * jnp.tanh(t)


def attend(query, keys, values, scale):
    count, wide = query.shape
    head = wide // 2
    if count > 128:
        halves = [slice(0, head), slice(head, wide)]
        return jnp.concatenate([blend(query[:, m], keys[:, m], values[:, m], scale) for m in halves], axis=1)
    none = jnp.zeros((count, head), query.dtype)
    upper = jnp.concatenate([query[:, :head], none], axis=1)
    lower = jnp.concatenate([none, query[:, head:]], axis=1)
    both = blend(jnp.concatenate([upper, lower], axis=0), keys, values, scale)
    return jnp.concatenate([both[:count, :head], both[count:, head:]], axis=1)


def blend(query, keys, values, scale):
    scores = lax.dot_general(
        query, keys, (((1,), (1,)), ((), ())), preferred_element_type=jnp.float32
    )
    t = scores * (0.5 * scale)
    weights = (t + t * jnp.tanh(t)).astype(jnp.bfloat16)
    return jnp.dot(weights, values, preferred_element_type=jnp.float32)


def spread_loop(count, body, together):
    def several(n, _):
        for m in range(together):
            body(n * together + m)
        return 0

    together = min(together, max(count, 1))
    whole = count // together
    if whole == 1:
        several(0, 0)
    elif whole:
        lax.fori_loop(0, whole, several, 0)
    for n in range(whole * together, count):
        body(n)


def seen(values, base, visible):
    rows = lax.broadcasted_iota(jnp.int32, values.shape, 0) + base
    return jnp.where(rows < visible, values, jnp.zeros_like(values))


def plan(shift, groups):
    far = min(shift, groups - shift) * 16 // groups
    if far <= 1:
        return PLANS["near"]
    return PLANS["mid" if far <= 5 else "far"]


def steps(text):
    return [(text[n], int(text[n + 1])) for n in range(0, len(text), 2)]


NEAR = "q0q1q2q3k0o0o1a0a1a2a3e0f0f1"
MID = "q0k0q1q2q3o0a0a1a2o1a3e0f0f1"
FAR = "q0k0q1o0q2q3a0a1a2o1a3e0f0f1"
LEAN = dict(q=1, o=1, a=1, t=1, f=1)
FULL = dict(q=2, o=1, a=4, t=4, f=2)
PLANS = dict(
    near=(2, dict(q=4, o=2, a=4, f=2), steps(NEAR), 4, LEAN),
    mid=(2, dict(q=4, o=2, a=4, f=2), steps(MID), 4, FULL | dict(f=1)),
    far=(4, dict(q=4, o=2, a=4, f=2), steps(FAR), 4, FULL),
)


def layer_kernel(
    shift, kv_heads, blocks, order, ahead, unroll,
    owner, counts, prefix_len, cand, cache, w, w_out, gain, out,
    tok, wq, kv, vm, pk, q, pq, ans, got, u, acc, wo, gn,
    w_sems, kv_sem, wo_sem, gn_sem,
    tok_send, tok_recv, pk_send, pk_recv, q_send, q_recv, a_send, a_recv,
):
    groups = lax.axis_size("group")
    helpers = lax.axis_size("helper")
    g = lax.axis_index("group")
    h = lax.axis_index("helper")
    slots, width = cand.shape
    length = cache.shape[1]
    head = width // HEADS
    scale = head ** (-0.5)
    chunks = blocks["q"]
    wide = 2 * head
    pairs = width // wide
    sent_pairs = kv_heads // 2
    q_pairs = pairs - sent_pairs
    q_width = q_pairs * wide
    others = list(range(1, helpers))
    user = lax.rem(g - shift + groups, groups)
    visible = prefix_len[user]
    live = counts[user] - h * slots

    loads = []
    for n, k in enumerate((2, 3, 1, 0)):
        cols = slice(k * width, (k + 1) * width)
        loads.append(pltpu.make_async_copy(w.at[:, cols], wq.at[k], w_sems.at[n]))
    loads[0].start()
    kv_load = pltpu.make_async_copy(cache, kv, kv_sem)
    kv_load.start()
    wo_load = pltpu.make_async_copy(w_out, wo, wo_sem)
    gn_load = pltpu.make_async_copy(gain, gn, gn_sem)

    barrier = pltpu.get_barrier_semaphore()
    greeted = [{"helper": lax.rem(h + away, helpers)} for away in others]
    if shift:
        target = lax.rem(g + shift, groups)
        greeted.append({"group": user})
    for friend in greeted:
        pl.semaphore_signal(barrier, inc=1, device_id=friend, device_id_type=MESH)
    pl.semaphore_wait(barrier, len(greeted))

    def part(c, kind="q"):
        size = slots // blocks[kind]
        return pl.ds(pl.multiple_of(c * size, size), size)

    def within(c, kind, finer):
        ratio = blocks[finer] // blocks[kind]
        return [c * ratio + m for m in range(ratio)]

    def token_copy(c):
        rows = part(c)
        if not shift:
            return pltpu.make_async_copy(cand.at[rows], tok.at[rows], tok_recv.at[c])
        return pltpu.make_async_remote_copy(
            cand.at[rows], tok.at[rows], tok_send.at[c], tok_recv.at[c],
            device_id={"group": target}, device_id_type=MESH,
        )

    for c in range(min(ahead, chunks)):
        token_copy(c).start()

    def kv_copy(n, away, kind):
        cols = slice(q_width + n * wide, q_width + (n + 1) * wide)
        here = slice(n * wide, (n + 1) * wide)
        return pltpu.make_async_remote_copy(
            cache.at[kind, :, cols], pk.at[away - 1, kind, :, here],
            pk_send.at[away - 1, kind, n], pk_recv.at[away - 1, kind, n],
            device_id={"helper": lax.rem(h + away, helpers)}, device_id_type=MESH,
        )

    kv_copies = [kv_copy(n, away, kind) for n in range(sent_pairs) for away in others for kind in (0, 1)]
    for copy in kv_copies:
        copy.start()

    def query_copy(away, c):
        rows = part(c)
        return pltpu.make_async_remote_copy(
            q.at[rows, 0:q_width], pq.at[away - 1, rows, :],
            q_send.at[away - 1, c], q_recv.at[away - 1, c],
            device_id={"helper": lax.rem(h + away, helpers)}, device_id_type=MESH,
        )

    def answer_copy(away, c):
        rows = part(c, "a")
        return pltpu.make_async_remote_copy(
            ans.at[away - 1, rows, :], got.at[away - 1, rows, :],
            a_send.at[away - 1, c], a_recv.at[away - 1, c],
            device_id={"helper": lax.rem(h - away + helpers, helpers)}, device_id_type=MESH,
        )

    def at_pair(n):
        return pl.ds(pl.multiple_of(n * wide, wide), wide)

    def project(k, rows, cols):
        return silu(jnp.dot(tok[rows, :], wq[k, :, cols], preferred_element_type=jnp.float32))

    def queries(c):
        rows = part(c)

        def body(n):
            cols = at_pair(n)
            q[rows, cols] = project(2, rows, cols).astype(jnp.bfloat16)

        spread_loop(pairs, body, unroll["q"])
        for away in others:
            query_copy(away, c).start()

    def own(b):
        rows = part(b, "o")

        def body(n):
            cols = at_pair(n)
            query = q[rows, cols]
            own_k = project(3, rows, cols).astype(jnp.bfloat16).astype(jnp.float32)
            own_v = project(1, rows, cols).astype(jnp.bfloat16).astype(jnp.float32)
            u[rows, cols] = project(0, rows, cols)
            prod = query.astype(jnp.float32) * own_k
            keys = kv[0, :, cols]
            values = vm[:, cols]
            mixed = attend(query, keys, values, scale)
            own_self = []
            for m in range(2):
                here = slice(m * head, (m + 1) * head)
                selfw = silu(jnp.sum(prod[:, here], axis=1, keepdims=True) * scale)
                selfw = selfw.astype(jnp.bfloat16).astype(jnp.float32)
                own_self.append(selfw * own_v[:, here])
            acc[rows, cols] = mixed + jnp.concatenate(own_self, axis=1)

        spread_loop(pairs, body, unroll["o"])

    def answers(c):
        rows = part(c, "a")
        for away in others:
            for piece in within(c, "a", "q"):
                query_copy(away, piece).wait_recv()

            def body(n):
                cols = at_pair(n)
                mixed = attend(pq[away - 1, rows, cols], kv[0, :, cols], vm[:, cols], scale)
                ans[away - 1, rows, cols] = mixed.astype(jnp.bfloat16)

            spread_loop(q_pairs, body, unroll["a"])
            answer_copy(away, c).start()

    def traveled(c):
        rows = part(c, "f")
        def body(n):
            here = at_pair(n)
            cols = at_pair(n + q_pairs)
            query = q[rows, cols]
            total = acc[rows, cols]
            for away in others:
                base = lax.rem(h - away + helpers, helpers) * length
                values = seen(pk[away - 1, 1, :, here], base, visible)
                total += attend(query, pk[away - 1, 0, :, here], values, scale)
            acc[rows, cols] = total

        spread_loop(sent_pairs, body, unroll["t"])

    def finish(c):
        rows = part(c, "f")
        size = slots // blocks["f"]
        if sent_pairs:
            traveled(c)
        for away in others:
            for piece in within(c, "f", "a"):
                answer_copy(away, piece).wait_recv()
        a = acc[rows, :]
        gate = u[rows, :]
        for away in others:
            extra = got[away - 1, rows, :].astype(jnp.float32)
            if sent_pairs:
                extra = jnp.concatenate([extra, jnp.zeros((size, width - q_width), jnp.float32)], axis=1)
            a += extra
        centre = a - jnp.mean(a, axis=-1, keepdims=True)
        spread = jnp.mean(centre * centre, axis=-1, keepdims=True)
        normed = (centre * lax.rsqrt(spread + EPS) * gn[...] * gate).astype(jnp.bfloat16)

        def body(n):
            cols = at_pair(n)
            result = jnp.dot(normed, wo[:, cols], preferred_element_type=jnp.float32)
            places = lax.broadcasted_iota(jnp.int32, result.shape, 0) + c * size
            out[rows, cols] = jnp.where(places < live, result, 0.0).astype(jnp.bfloat16)

        spread_loop(pairs, body, unroll["f"])

    def mask(n, _):
        cols = at_pair(n)
        vm[:, cols] = seen(kv[1, :, cols], h * length, visible)
        return 0

    def at_queries(c):
        @pl.when(c == 0)
        def _():
            loads[0].wait()
            for load in loads[1:] + [wo_load, gn_load]:
                load.start()

        token_copy(c).wait_recv() if shift else token_copy(c).wait()
        if ahead < chunks:
            pl.when(c + ahead < chunks)(lambda: token_copy(c + ahead).start())
        queries(c)

    def at_first(_):
        kv_load.wait()
        lax.fori_loop(0, pairs, mask, 0)
        for load in loads[1:]:
            load.wait()

    def at_end(_):
        for copy in kv_copies:
            copy.wait_recv()
        wo_load.wait()
        gn_load.wait()

    work = dict(q=at_queries, k=at_first, o=own, a=answers, e=at_end, f=finish)

    def step(t, _):
        for kind, run in work.items():
            places = [(n, c) for n, (name, c) in enumerate(order) if name == kind]
            here = functools.reduce(jnp.logical_or, [t == n for n, _ in places])
            index = sum(jnp.where(t == n, c, 0) for n, c in places)
            pl.when(here)(functools.partial(run, index))
        return 0

    lax.fori_loop(0, len(order), step, 0)

    def drain(kind, copies):
        def body(c, _):
            copies(c)
            return 0

        lax.fori_loop(0, blocks[kind], body, 0)

    def sent(c):
        if shift:
            token_copy(c).wait_send()
        for away in others:
            query_copy(away, c).wait_send()

    drain("q", sent)
    drain("a", lambda c: [answer_copy(away, c).wait_send() for away in others])
    for copy in kv_copies:
        copy.wait_send()


def layer(shift, groups, helpers, owner, counts, prefix_len, cand, cache, w, w_out, gain):
    slots, width = cand.shape
    length = cache.shape[1]
    kv_heads, blocks, order, ahead, unroll = plan(shift, groups)
    chunks = blocks["q"]
    q_width = width - kv_heads * (width // HEADS)
    pieces = helpers - 1
    kv_width = max(width - q_width, 128)
    dma = pltpu.SemaphoreType.DMA
    smem = pl.BlockSpec(memory_space=pltpu.SMEM)
    anywhere = pl.BlockSpec(memory_space=pl.ANY)
    bf16, f32 = jnp.bfloat16, jnp.float32
    return pl.pallas_call(
        functools.partial(layer_kernel, shift, kv_heads, blocks, order, ahead, unroll),
        in_specs=[smem] * 3 + [anywhere] * 5,
        out_specs=pl.BlockSpec(memory_space=pltpu.VMEM),
        out_shape=jax.ShapeDtypeStruct((slots, width), bf16),
        scratch_shapes=[
            pltpu.VMEM((slots, width), bf16),
            pltpu.VMEM((4, width, width), bf16),
            pltpu.VMEM((2, length, width), bf16),
            pltpu.VMEM((length, width), bf16),
            pltpu.VMEM((pieces, 2, length, kv_width), bf16),
            pltpu.VMEM((slots, width), bf16),
            pltpu.VMEM((pieces, slots, q_width), bf16),
            pltpu.VMEM((pieces, slots, q_width), bf16),
            pltpu.VMEM((pieces, slots, q_width), bf16),
            pltpu.VMEM((slots, width), f32),
            pltpu.VMEM((slots, width), f32),
            pltpu.VMEM((width, width), bf16),
            pltpu.VMEM((1, width), f32),
            dma((4,)), dma(()), dma(()), dma(()),
            dma((chunks,)), dma((chunks,)),
            dma((pieces, 2, max(kv_heads // 2, 1))), dma((pieces, 2, max(kv_heads // 2, 1))),
            dma((pieces, chunks)), dma((pieces, chunks)),
            dma((pieces, blocks["a"])), dma((pieces, blocks["a"])),
        ],
        compiler_params=pltpu.CompilerParams(
            collective_id=shift, has_side_effects=True, vmem_limit_bytes=60 * 1024 * 1024
        ),
        name="layer",
    )(owner, counts, prefix_len, cand, cache, w, w_out, gain)


def local(candidates, prefix_cache, w_uvqk, w_output, norm_gain, owner, counts, prefix_len):
    groups = lax.axis_size("group")
    helpers = lax.axis_size("helper")
    _, slots, width = candidates.shape
    length = prefix_cache.shape[2]
    cache = prefix_cache.reshape(2, length, width)
    branches = [functools.partial(layer, s, groups, helpers) for s in range(groups)]
    result = lax.switch(
        owner[0], branches, owner, counts, prefix_len,
        candidates[0], cache, w_uvqk, w_output, norm_gain.reshape(1, width),
    )
    return result[None]


def solution(mesh):
    in_specs = (
        P("group", "helper", None),
        P("group", None, "helper", None),
        P(),
        P(),
        P(),
        P(),
        P(),
        P(),
    )
    out_specs = P("group", "helper", None)
    return jax.shard_map(local, mesh=mesh, in_specs=in_specs, out_specs=out_specs, check_vma=False)
```

```python
import functools

import jax
import jax.numpy as jnp
from jax import lax
from jax.experimental import pallas as pl
from jax.experimental.pallas import tpu as pltpu
from jax.sharding import PartitionSpec as P

HEADS = 8
EPS = 1e-05
MESH = pl.DeviceIdType.MESH


def silu(v):
    t = v * 0.5
    return t + t * jnp.tanh(t)


def attend(query, keys, values, scale):
    count, wide = query.shape
    head = wide // 2
    if count > 128:
        halves = [slice(0, head), slice(head, wide)]
        return jnp.concatenate([blend(query[:, m], keys[:, m], values[:, m], scale) for m in halves], axis=1)
    none = jnp.zeros((count, head), query.dtype)
    upper = jnp.concatenate([query[:, :head], none], axis=1)
    lower = jnp.concatenate([none, query[:, head:]], axis=1)
    both = blend(jnp.concatenate([upper, lower], axis=0), keys, values, scale)
    return jnp.concatenate([both[:count, :head], both[count:, head:]], axis=1)


def blend(query, keys, values, scale):
    scores = lax.dot_general(
        query, keys, (((1,), (1,)), ((), ())), preferred_element_type=jnp.float32
    )
    t = scores * (0.5 * scale)
    weights = (t + t * jnp.tanh(t)).astype(jnp.bfloat16)
    return jnp.dot(weights, values, preferred_element_type=jnp.float32)


def spread_loop(count, body, together, sent=None):
    def several(n, _):
        for m in range(together):
            body(n * together + m)
        if sent is not None:
            last, send = sent
            pl.when(n == (last - 1) // together)(send)
        return 0

    together = min(together, max(count, 1))
    whole = count // together
    if whole == 1 and sent is None:
        several(0, 0)
    elif whole:
        lax.fori_loop(0, whole, several, 0)
    for n in range(whole * together, count):
        body(n)


def seen(values, base, visible):
    rows = lax.broadcasted_iota(jnp.int32, values.shape, 0) + base
    return jnp.where(rows < visible, values, jnp.zeros_like(values))


def plan(shift, groups):
    far = min(shift, groups - shift) * 16 // groups
    if far <= 1:
        return PLANS["near"]
    return PLANS["mid" if far <= 5 else "far"]


def steps(text):
    return [(text[n], int(text[n + 1])) for n in range(0, len(text), 2)]


NEAR = "q0q1q2q3k0o0a0a1a2a3o1e0f0f1"
MID = "q0k0q1q2q3a0o0a1a2a3o1e0f0f1"
FAR = "q0k0q1o0q2q3a0a1a2a3o1e0f0f1"
LEAN = dict(q=1, o=1, a=1, t=1, f=1)
FULL = dict(q=2, o=1, a=4, t=4, f=2)
PLANS = dict(
    near=(2, dict(q=4, o=2, a=4, f=2), steps(NEAR), 4, LEAN),
    mid=(2, dict(q=4, o=2, a=4, f=2), steps(MID), 4, FULL),
    far=(4, dict(q=4, o=2, a=4, f=2), steps(FAR), 4, FULL),
)


def layer_kernel(
    shift, kv_heads, blocks, order, ahead, unroll,
    owner, counts, prefix_len, cand, cache, w, w_out, gain, out,
    tok, wq, kv, vm, pk, q, pq, ans, got, u, acc, wo, gn,
    w_sems, kv_sem, wo_sem, gn_sem,
    tok_send, tok_recv, pk_send, pk_recv, q_send, q_recv, a_send, a_recv,
):
    groups = lax.axis_size("group")
    helpers = lax.axis_size("helper")
    g = lax.axis_index("group")
    h = lax.axis_index("helper")
    slots, width = cand.shape
    length = cache.shape[1]
    head = width // HEADS
    scale = head ** (-0.5)
    chunks = blocks["q"]
    wide = 2 * head
    pairs = width // wide
    sent_pairs = kv_heads // 2
    q_pairs = pairs - sent_pairs
    q_width = q_pairs * wide
    others = list(range(1, helpers))
    user = lax.rem(g - shift + groups, groups)
    visible = prefix_len[user]
    live = counts[user] - h * slots

    loads = []
    for n, k in enumerate((2, 3, 1, 0)):
        cols = slice(k * width, (k + 1) * width)
        loads.append(pltpu.make_async_copy(w.at[:, cols], wq.at[k], w_sems.at[n]))
    loads[0].start()
    kv_load = pltpu.make_async_copy(cache, kv, kv_sem)
    kv_load.start()
    wo_load = pltpu.make_async_copy(w_out, wo, wo_sem)
    gn_load = pltpu.make_async_copy(gain, gn, gn_sem)

    barrier = pltpu.get_barrier_semaphore()
    greeted = [{"helper": lax.rem(h + away, helpers)} for away in others]
    if shift:
        target = lax.rem(g + shift, groups)
        greeted.append({"group": user})
    for friend in greeted:
        pl.semaphore_signal(barrier, inc=1, device_id=friend, device_id_type=MESH)
    pl.semaphore_wait(barrier, len(greeted))

    def part(c, kind="q"):
        size = slots // blocks[kind]
        return pl.ds(pl.multiple_of(c * size, size), size)

    def within(c, kind, finer):
        ratio = blocks[finer] // blocks[kind]
        return [c * ratio + m for m in range(ratio)]

    def token_copy(c):
        rows = part(c)
        if not shift:
            return pltpu.make_async_copy(cand.at[rows], tok.at[rows], tok_recv.at[c])
        return pltpu.make_async_remote_copy(
            cand.at[rows], tok.at[rows], tok_send.at[c], tok_recv.at[c],
            device_id={"group": target}, device_id_type=MESH,
        )

    for c in range(min(ahead, chunks)):
        token_copy(c).start()

    def kv_copy(n, away, kind):
        cols = slice(q_width + n * wide, q_width + (n + 1) * wide)
        here = slice(n * wide, (n + 1) * wide)
        return pltpu.make_async_remote_copy(
            cache.at[kind, :, cols], pk.at[away - 1, kind, :, here],
            pk_send.at[away - 1, kind, n], pk_recv.at[away - 1, kind, n],
            device_id={"helper": lax.rem(h + away, helpers)}, device_id_type=MESH,
        )

    kv_copies = [kv_copy(n, away, kind) for n in range(sent_pairs) for away in others for kind in (0, 1)]
    for copy in kv_copies:
        copy.start()

    def query_copy(away, c):
        rows = part(c)
        return pltpu.make_async_remote_copy(
            q.at[rows, 0:q_width], pq.at[away - 1, rows, :],
            q_send.at[away - 1, c], q_recv.at[away - 1, c],
            device_id={"helper": lax.rem(h + away, helpers)}, device_id_type=MESH,
        )

    def answer_copy(away, c):
        rows = part(c, "a")
        return pltpu.make_async_remote_copy(
            ans.at[away - 1, rows, :], got.at[away - 1, rows, :],
            a_send.at[away - 1, c], a_recv.at[away - 1, c],
            device_id={"helper": lax.rem(h - away + helpers, helpers)}, device_id_type=MESH,
        )

    def at_pair(n):
        return pl.ds(pl.multiple_of(n * wide, wide), wide)

    def project(k, rows, cols):
        return silu(jnp.dot(tok[rows, :], wq[k, :, cols], preferred_element_type=jnp.float32))

    def queries(c):
        rows = part(c)

        def body(n):
            cols = at_pair(n)
            q[rows, cols] = project(2, rows, cols).astype(jnp.bfloat16)

        def send():
            for away in others:
                query_copy(away, c).start()

        spread_loop(pairs, body, unroll["q"], (q_pairs, send))

    def own(b):
        rows = part(b, "o")

        def body(n):
            cols = at_pair(n)
            query = q[rows, cols]
            own_k = project(3, rows, cols).astype(jnp.bfloat16).astype(jnp.float32)
            own_v = project(1, rows, cols).astype(jnp.bfloat16).astype(jnp.float32)
            u[rows, cols] = project(0, rows, cols)
            prod = query.astype(jnp.float32) * own_k
            keys = kv[0, :, cols]
            values = vm[:, cols]
            mixed = attend(query, keys, values, scale)
            own_self = []
            for m in range(2):
                here = slice(m * head, (m + 1) * head)
                selfw = silu(jnp.sum(prod[:, here], axis=1, keepdims=True) * scale)
                selfw = selfw.astype(jnp.bfloat16).astype(jnp.float32)
                own_self.append(selfw * own_v[:, here])
            acc[rows, cols] = mixed + jnp.concatenate(own_self, axis=1)

        spread_loop(pairs, body, unroll["o"])

    def answers(c):
        rows = part(c, "a")
        for away in others:
            for piece in within(c, "a", "q"):
                query_copy(away, piece).wait_recv()

            def body(n):
                cols = at_pair(n)
                mixed = attend(pq[away - 1, rows, cols], kv[0, :, cols], vm[:, cols], scale)
                ans[away - 1, rows, cols] = mixed.astype(jnp.bfloat16)

            spread_loop(q_pairs, body, unroll["a"])
            answer_copy(away, c).start()

    def traveled(c):
        rows = part(c, "f")
        def body(n):
            here = at_pair(n)
            cols = at_pair(n + q_pairs)
            query = q[rows, cols]
            total = acc[rows, cols]
            for away in others:
                base = lax.rem(h - away + helpers, helpers) * length
                values = seen(pk[away - 1, 1, :, here], base, visible)
                total += attend(query, pk[away - 1, 0, :, here], values, scale)
            acc[rows, cols] = total

        spread_loop(sent_pairs, body, unroll["t"])

    def finish(c):
        rows = part(c, "f")
        size = slots // blocks["f"]
        if sent_pairs:
            traveled(c)
        for away in others:
            for piece in within(c, "f", "a"):
                answer_copy(away, piece).wait_recv()
        a = acc[rows, :]
        gate = u[rows, :]
        for away in others:
            extra = got[away - 1, rows, :].astype(jnp.float32)
            if sent_pairs:
                extra = jnp.concatenate([extra, jnp.zeros((size, width - q_width), jnp.float32)], axis=1)
            a += extra
        centre = a - jnp.mean(a, axis=-1, keepdims=True)
        spread = jnp.mean(centre * centre, axis=-1, keepdims=True)
        normed = (centre * lax.rsqrt(spread + EPS) * gn[...] * gate).astype(jnp.bfloat16)

        def body(n):
            cols = at_pair(n)
            result = jnp.dot(normed, wo[:, cols], preferred_element_type=jnp.float32)
            places = lax.broadcasted_iota(jnp.int32, result.shape, 0) + c * size
            out[rows, cols] = jnp.where(places < live, result, 0.0).astype(jnp.bfloat16)

        spread_loop(pairs, body, unroll["f"])

    def mask(n, _):
        cols = at_pair(n)
        vm[:, cols] = seen(kv[1, :, cols], h * length, visible)
        return 0

    def at_queries(c):
        @pl.when(c == 0)
        def _():
            loads[0].wait()
            for load in loads[1:] + [wo_load, gn_load]:
                load.start()

        token_copy(c).wait_recv() if shift else token_copy(c).wait()
        if ahead < chunks:
            pl.when(c + ahead < chunks)(lambda: token_copy(c + ahead).start())
        queries(c)

    def at_first(_):
        kv_load.wait()
        lax.fori_loop(0, pairs, mask, 0)
        for load in loads[1:]:
            load.wait()

    def at_end(_):
        for copy in kv_copies:
            copy.wait_recv()
        wo_load.wait()
        gn_load.wait()

    work = dict(q=at_queries, k=at_first, o=own, a=answers, e=at_end, f=finish)

    def step(t, _):
        for kind, run in work.items():
            places = [(n, c) for n, (name, c) in enumerate(order) if name == kind]
            here = functools.reduce(jnp.logical_or, [t == n for n, _ in places])
            index = sum(jnp.where(t == n, c, 0) for n, c in places)
            pl.when(here)(functools.partial(run, index))
        return 0

    lax.fori_loop(0, len(order), step, 0)

    def drain(kind, copies):
        def body(c, _):
            copies(c)
            return 0

        lax.fori_loop(0, blocks[kind], body, 0)

    def sent(c):
        if shift:
            token_copy(c).wait_send()
        for away in others:
            query_copy(away, c).wait_send()

    drain("q", sent)
    drain("a", lambda c: [answer_copy(away, c).wait_send() for away in others])
    for copy in kv_copies:
        copy.wait_send()


def layer(shift, groups, helpers, owner, counts, prefix_len, cand, cache, w, w_out, gain):
    slots, width = cand.shape
    length = cache.shape[1]
    kv_heads, blocks, order, ahead, unroll = plan(shift, groups)
    chunks = blocks["q"]
    q_width = width - kv_heads * (width // HEADS)
    pieces = helpers - 1
    kv_width = max(width - q_width, 128)
    dma = pltpu.SemaphoreType.DMA
    smem = pl.BlockSpec(memory_space=pltpu.SMEM)
    anywhere = pl.BlockSpec(memory_space=pl.ANY)
    bf16, f32 = jnp.bfloat16, jnp.float32
    return pl.pallas_call(
        functools.partial(layer_kernel, shift, kv_heads, blocks, order, ahead, unroll),
        in_specs=[smem] * 3 + [anywhere] * 5,
        out_specs=pl.BlockSpec(memory_space=pltpu.VMEM),
        out_shape=jax.ShapeDtypeStruct((slots, width), bf16),
        scratch_shapes=[
            pltpu.VMEM((slots, width), bf16),
            pltpu.VMEM((4, width, width), bf16),
            pltpu.VMEM((2, length, width), bf16),
            pltpu.VMEM((length, width), bf16),
            pltpu.VMEM((pieces, 2, length, kv_width), bf16),
            pltpu.VMEM((slots, width), bf16),
            pltpu.VMEM((pieces, slots, q_width), bf16),
            pltpu.VMEM((pieces, slots, q_width), bf16),
            pltpu.VMEM((pieces, slots, q_width), bf16),
            pltpu.VMEM((slots, width), f32),
            pltpu.VMEM((slots, width), f32),
            pltpu.VMEM((width, width), bf16),
            pltpu.VMEM((1, width), f32),
            dma((4,)), dma(()), dma(()), dma(()),
            dma((chunks,)), dma((chunks,)),
            dma((pieces, 2, max(kv_heads // 2, 1))), dma((pieces, 2, max(kv_heads // 2, 1))),
            dma((pieces, chunks)), dma((pieces, chunks)),
            dma((pieces, blocks["a"])), dma((pieces, blocks["a"])),
        ],
        compiler_params=pltpu.CompilerParams(
            collective_id=shift, has_side_effects=True, vmem_limit_bytes=60 * 1024 * 1024,
        ),
        name="layer",
    )(owner, counts, prefix_len, cand, cache, w, w_out, gain)


def local(candidates, prefix_cache, w_uvqk, w_output, norm_gain, owner, counts, prefix_len):
    groups = lax.axis_size("group")
    helpers = lax.axis_size("helper")
    _, slots, width = candidates.shape
    length = prefix_cache.shape[2]
    cache = prefix_cache.reshape(2, length, width)
    branches = [functools.partial(layer, s, groups, helpers) for s in range(groups)]
    result = lax.switch(
        owner[0], branches, owner, counts, prefix_len,
        candidates[0], cache, w_uvqk, w_output, norm_gain.reshape(1, width),
    )
    return result[None]


def solution(mesh):
    in_specs = (
        P("group", "helper", None),
        P("group", None, "helper", None),
        P(),
        P(),
        P(),
        P(),
        P(),
        P(),
    )
    out_specs = P("group", "helper", None)
    return jax.shard_map(local, mesh=mesh, in_specs=in_specs, out_specs=out_specs, check_vma=False)
```

```python
import functools

import jax
import jax.numpy as jnp
from jax import lax
from jax.experimental import pallas as pl
from jax.experimental.pallas import tpu as pltpu
from jax.sharding import PartitionSpec as P

HEADS = 8
EPS = 1e-05
MESH = pl.DeviceIdType.MESH


def silu(v):
    t = v * 0.5
    return t + t * jnp.tanh(t)


def attend(query, keys, values, scale):
    count, wide = query.shape
    head = wide // 2
    if count > 128:
        halves = [slice(0, head), slice(head, wide)]
        return jnp.concatenate([blend(query[:, m], keys[:, m], values[:, m], scale) for m in halves], axis=1)
    none = jnp.zeros((count, head), query.dtype)
    upper = jnp.concatenate([query[:, :head], none], axis=1)
    lower = jnp.concatenate([none, query[:, head:]], axis=1)
    both = blend(jnp.concatenate([upper, lower], axis=0), keys, values, scale)
    return jnp.concatenate([both[:count, :head], both[count:, head:]], axis=1)


def blend(query, keys, values, scale):
    scores = lax.dot_general(
        query, keys, (((1,), (1,)), ((), ())), preferred_element_type=jnp.float32
    )
    t = scores * (0.5 * scale)
    weights = (t + t * jnp.tanh(t)).astype(jnp.bfloat16)
    return jnp.dot(weights, values, preferred_element_type=jnp.float32)


def spread_loop(count, body, together, sent=None):
    def several(n, _):
        for m in range(together):
            body(n * together + m)
        if sent is not None:
            last, send = sent
            pl.when(n == (last - 1) // together)(send)
        return 0

    together = min(together, max(count, 1))
    whole = count // together
    if whole == 1 and sent is None:
        several(0, 0)
    elif whole:
        lax.fori_loop(0, whole, several, 0)
    for n in range(whole * together, count):
        body(n)


def seen(values, base, visible):
    rows = lax.broadcasted_iota(jnp.int32, values.shape, 0) + base
    return jnp.where(rows < visible, values, jnp.zeros_like(values))


def plan(shift, groups):
    far = min(shift, groups - shift) * 16 // groups
    if far <= 1:
        return PLANS["near"]
    return PLANS["mid" if far <= 5 else "far"]


def steps(text):
    return [(text[n], int(text[n + 1])) for n in range(0, len(text), 2)]


NEAR = "q0q1q2q3k0o0a0a1a2a3o1e0f0f1"
MID = "q0k0q1q2q3a0o0a1a2a3o1e0f0f1"
FAR = "q0k0q1o0q2q3a0a1o1e0f0f1"
LEAN = dict(q=1, o=1, a=1, t=1, f=1)
FULL = dict(q=2, o=1, a=4, t=4, f=2)
PLANS = dict(
    near=(2, dict(q=4, o=2, a=4, f=2), steps(NEAR), 4, LEAN),
    mid=(2, dict(q=4, o=2, a=4, f=2), steps(MID), 4, FULL),
    far=(4, dict(q=4, o=2, a=2, f=2), steps(FAR), 4, FULL | dict(f=4)),
)


def layer_kernel(
    shift, kv_heads, blocks, order, ahead, unroll,
    owner, counts, prefix_len, cand, cache, w, w_out, gain, out,
    tok, wq, kv, vm, pk, q, pq, ans, got, u, acc, wo, gn,
    w_sems, kv_sem, wo_sem, gn_sem,
    tok_send, tok_recv, pk_send, pk_recv, q_send, q_recv, a_send, a_recv,
):
    groups = lax.axis_size("group")
    helpers = lax.axis_size("helper")
    g = lax.axis_index("group")
    h = lax.axis_index("helper")
    slots, width = cand.shape
    length = cache.shape[1]
    head = width // HEADS
    scale = head ** (-0.5)
    chunks = blocks["q"]
    wide = 2 * head
    pairs = width // wide
    sent_pairs = kv_heads // 2
    q_pairs = pairs - sent_pairs
    q_width = q_pairs * wide
    others = list(range(1, helpers))
    user = lax.rem(g - shift + groups, groups)
    visible = prefix_len[user]
    live = counts[user] - h * slots

    loads = []
    for n, k in enumerate((2, 3, 1, 0)):
        cols = slice(k * width, (k + 1) * width)
        loads.append(pltpu.make_async_copy(w.at[:, cols], wq.at[k], w_sems.at[n]))
    loads[0].start()
    kv_load = pltpu.make_async_copy(cache, kv, kv_sem)
    kv_load.start()
    wo_load = pltpu.make_async_copy(w_out, wo, wo_sem)
    gn_load = pltpu.make_async_copy(gain, gn, gn_sem)

    barrier = pltpu.get_barrier_semaphore()
    greeted = [{"helper": lax.rem(h + away, helpers)} for away in others]
    if shift:
        target = lax.rem(g + shift, groups)
        greeted.append({"group": user})
    for friend in greeted:
        pl.semaphore_signal(barrier, inc=1, device_id=friend, device_id_type=MESH)
    pl.semaphore_wait(barrier, len(greeted))

    def part(c, kind="q"):
        size = slots // blocks[kind]
        return pl.ds(pl.multiple_of(c * size, size), size)

    def within(c, kind, finer):
        ratio = blocks[finer] // blocks[kind]
        return [c * ratio + m for m in range(ratio)]

    def token_copy(c):
        rows = part(c)
        if not shift:
            return pltpu.make_async_copy(cand.at[rows], tok.at[rows], tok_recv.at[c])
        return pltpu.make_async_remote_copy(
            cand.at[rows], tok.at[rows], tok_send.at[c], tok_recv.at[c],
            device_id={"group": target}, device_id_type=MESH,
        )

    for c in range(min(ahead, chunks)):
        token_copy(c).start()

    def kv_copy(n, away, kind):
        cols = slice(q_width + n * wide, q_width + (n + 1) * wide)
        here = slice(n * wide, (n + 1) * wide)
        return pltpu.make_async_remote_copy(
            cache.at[kind, :, cols], pk.at[away - 1, kind, :, here],
            pk_send.at[away - 1, kind, n], pk_recv.at[away - 1, kind, n],
            device_id={"helper": lax.rem(h + away, helpers)}, device_id_type=MESH,
        )

    kv_copies = [kv_copy(n, away, kind) for n in range(sent_pairs) for away in others for kind in (0, 1)]
    for copy in kv_copies:
        copy.start()

    def query_copy(away, c):
        rows = part(c)
        return pltpu.make_async_remote_copy(
            q.at[rows, 0:q_width], pq.at[away - 1, rows, :],
            q_send.at[away - 1, c], q_recv.at[away - 1, c],
            device_id={"helper": lax.rem(h + away, helpers)}, device_id_type=MESH,
        )

    def answer_copy(away, c):
        rows = part(c, "a")
        return pltpu.make_async_remote_copy(
            ans.at[away - 1, rows, :], got.at[away - 1, rows, :],
            a_send.at[away - 1, c], a_recv.at[away - 1, c],
            device_id={"helper": lax.rem(h - away + helpers, helpers)}, device_id_type=MESH,
        )

    def at_pair(n):
        return pl.ds(pl.multiple_of(n * wide, wide), wide)

    def project(k, rows, cols):
        return silu(jnp.dot(tok[rows, :], wq[k, :, cols], preferred_element_type=jnp.float32))

    def queries(c):
        rows = part(c)

        def body(n):
            cols = at_pair(n)
            q[rows, cols] = project(2, rows, cols).astype(jnp.bfloat16)

        def send():
            for away in others:
                query_copy(away, c).start()

        spread_loop(pairs, body, unroll["q"], (q_pairs, send))

    def own(b):
        rows = part(b, "o")

        def body(n):
            cols = at_pair(n)
            query = q[rows, cols]
            own_k = project(3, rows, cols).astype(jnp.bfloat16).astype(jnp.float32)
            own_v = project(1, rows, cols).astype(jnp.bfloat16).astype(jnp.float32)
            u[rows, cols] = project(0, rows, cols)
            prod = query.astype(jnp.float32) * own_k
            keys = kv[0, :, cols]
            values = vm[:, cols]
            mixed = attend(query, keys, values, scale)
            own_self = []
            for m in range(2):
                here = slice(m * head, (m + 1) * head)
                selfw = silu(jnp.sum(prod[:, here], axis=1, keepdims=True) * scale)
                selfw = selfw.astype(jnp.bfloat16).astype(jnp.float32)
                own_self.append(selfw * own_v[:, here])
            acc[rows, cols] = mixed + jnp.concatenate(own_self, axis=1)

        spread_loop(pairs, body, unroll["o"])

    def answers(c):
        rows = part(c, "a")
        for away in others:
            for piece in within(c, "a", "q"):
                query_copy(away, piece).wait_recv()

            def body(n):
                cols = at_pair(n)
                mixed = attend(pq[away - 1, rows, cols], kv[0, :, cols], vm[:, cols], scale)
                ans[away - 1, rows, cols] = mixed.astype(jnp.bfloat16)

            spread_loop(q_pairs, body, unroll["a"])
            answer_copy(away, c).start()

    def traveled(c):
        rows = part(c, "f")
        def body(n):
            here = at_pair(n)
            cols = at_pair(n + q_pairs)
            query = q[rows, cols]
            total = acc[rows, cols]
            for away in others:
                base = lax.rem(h - away + helpers, helpers) * length
                values = seen(pk[away - 1, 1, :, here], base, visible)
                total += attend(query, pk[away - 1, 0, :, here], values, scale)
            acc[rows, cols] = total

        spread_loop(sent_pairs, body, unroll["t"])

    def finish(c):
        rows = part(c, "f")
        size = slots // blocks["f"]
        if sent_pairs:
            traveled(c)
        for away in others:
            for piece in within(c, "f", "a"):
                answer_copy(away, piece).wait_recv()
        a = acc[rows, :]
        gate = u[rows, :]
        for away in others:
            extra = got[away - 1, rows, :].astype(jnp.float32)
            if sent_pairs:
                extra = jnp.concatenate([extra, jnp.zeros((size, width - q_width), jnp.float32)], axis=1)
            a += extra
        centre = a - jnp.mean(a, axis=-1, keepdims=True)
        spread = jnp.mean(centre * centre, axis=-1, keepdims=True)
        normed = (centre * lax.rsqrt(spread + EPS) * gn[...] * gate).astype(jnp.bfloat16)

        def body(n):
            cols = at_pair(n)
            result = jnp.dot(normed, wo[:, cols], preferred_element_type=jnp.float32)
            places = lax.broadcasted_iota(jnp.int32, result.shape, 0) + c * size
            out[rows, cols] = jnp.where(places < live, result, 0.0).astype(jnp.bfloat16)

        spread_loop(pairs, body, unroll["f"])

    def mask(n, _):
        cols = at_pair(n)
        vm[:, cols] = seen(kv[1, :, cols], h * length, visible)
        return 0

    def at_queries(c):
        @pl.when(c == 0)
        def _():
            loads[0].wait()
            for load in loads[1:] + [wo_load, gn_load]:
                load.start()

        token_copy(c).wait_recv() if shift else token_copy(c).wait()
        if ahead < chunks:
            pl.when(c + ahead < chunks)(lambda: token_copy(c + ahead).start())
        queries(c)

    def at_first(_):
        kv_load.wait()
        lax.fori_loop(0, pairs, mask, 0)
        for load in loads[1:]:
            load.wait()

    def at_end(_):
        for copy in kv_copies:
            copy.wait_recv()
        wo_load.wait()
        gn_load.wait()

    work = dict(q=at_queries, k=at_first, o=own, a=answers, e=at_end, f=finish)

    def step(t, _):
        for kind, run in work.items():
            places = [(n, c) for n, (name, c) in enumerate(order) if name == kind]
            here = functools.reduce(jnp.logical_or, [t == n for n, _ in places])
            index = sum(jnp.where(t == n, c, 0) for n, c in places)
            pl.when(here)(functools.partial(run, index))
        return 0

    lax.fori_loop(0, len(order), step, 0)

    def drain(kind, copies):
        def body(c, _):
            copies(c)
            return 0

        lax.fori_loop(0, blocks[kind], body, 0)

    def sent(c):
        if shift:
            token_copy(c).wait_send()
        for away in others:
            query_copy(away, c).wait_send()

    drain("q", sent)
    drain("a", lambda c: [answer_copy(away, c).wait_send() for away in others])
    for copy in kv_copies:
        copy.wait_send()


def layer(shift, groups, helpers, owner, counts, prefix_len, cand, cache, w, w_out, gain):
    slots, width = cand.shape
    length = cache.shape[1]
    kv_heads, blocks, order, ahead, unroll = plan(shift, groups)
    chunks = blocks["q"]
    q_width = width - kv_heads * (width // HEADS)
    pieces = helpers - 1
    kv_width = max(width - q_width, 128)
    dma = pltpu.SemaphoreType.DMA
    smem = pl.BlockSpec(memory_space=pltpu.SMEM)
    anywhere = pl.BlockSpec(memory_space=pl.ANY)
    bf16, f32 = jnp.bfloat16, jnp.float32
    return pl.pallas_call(
        functools.partial(layer_kernel, shift, kv_heads, blocks, order, ahead, unroll),
        in_specs=[smem] * 3 + [anywhere] * 5,
        out_specs=pl.BlockSpec(memory_space=pltpu.VMEM),
        out_shape=jax.ShapeDtypeStruct((slots, width), bf16),
        scratch_shapes=[
            pltpu.VMEM((slots, width), bf16),
            pltpu.VMEM((4, width, width), bf16),
            pltpu.VMEM((2, length, width), bf16),
            pltpu.VMEM((length, width), bf16),
            pltpu.VMEM((pieces, 2, length, kv_width), bf16),
            pltpu.VMEM((slots, width), bf16),
            pltpu.VMEM((pieces, slots, q_width), bf16),
            pltpu.VMEM((pieces, slots, q_width), bf16),
            pltpu.VMEM((pieces, slots, q_width), bf16),
            pltpu.VMEM((slots, width), f32),
            pltpu.VMEM((slots, width), f32),
            pltpu.VMEM((width, width), bf16),
            pltpu.VMEM((1, width), f32),
            dma((4,)), dma(()), dma(()), dma(()),
            dma((chunks,)), dma((chunks,)),
            dma((pieces, 2, max(kv_heads // 2, 1))), dma((pieces, 2, max(kv_heads // 2, 1))),
            dma((pieces, chunks)), dma((pieces, chunks)),
            dma((pieces, blocks["a"])), dma((pieces, blocks["a"])),
        ],
        compiler_params=pltpu.CompilerParams(
            collective_id=shift, has_side_effects=True, vmem_limit_bytes=60 * 1024 * 1024,
        ),
        name="layer",
    )(owner, counts, prefix_len, cand, cache, w, w_out, gain)


def local(candidates, prefix_cache, w_uvqk, w_output, norm_gain, owner, counts, prefix_len):
    groups = lax.axis_size("group")
    helpers = lax.axis_size("helper")
    _, slots, width = candidates.shape
    length = prefix_cache.shape[2]
    cache = prefix_cache.reshape(2, length, width)
    branches = [functools.partial(layer, s, groups, helpers) for s in range(groups)]
    result = lax.switch(
        owner[0], branches, owner, counts, prefix_len,
        candidates[0], cache, w_uvqk, w_output, norm_gain.reshape(1, width),
    )
    return result[None]


def solution(mesh):
    in_specs = (
        P("group", "helper", None),
        P("group", None, "helper", None),
        P(),
        P(),
        P(),
        P(),
        P(),
        P(),
    )
    out_specs = P("group", "helper", None)
    return jax.shard_map(local, mesh=mesh, in_specs=in_specs, out_specs=out_specs, check_vma=False)
```
